32 devices in a mesh: ctx: 16 (over z, x, core), tp: 2 (over y).
Axes of the slice: x: 2, y: 2, z: 4, core: 2. Of those that a mesh axis runs over, the one named last changes fastest.
Arguments:
- queries: bfloat16 [4096, 12288], P(('ctx', 'tp')), may hold values from -64 to 64
- keys: bfloat16 [4096, 1024], P(('ctx', 'tp')), may hold values from -4 to 4
- values: bfloat16 [4096, 1024], P(('ctx', 'tp')), may hold values from -6 to 6
- block_order: int32 [16], replicated, may hold values from 0 to 15, each once
Outputs:
- attended: bfloat16 [4096, 12288], P(('ctx', 'tp'))
The draws below stay inside these ranges and needn't reach their ends.
Inputs may be any that keep to these rules, and one draw needn't show every extreme that they name: A permutation: block r holds sequence span block_order[r] in its first 128 rows and span 2 * 16 - 1 - block_order[r] in its last 128 rows.
All inputs are finite; a program needn't handle non-finite values.
Results may differ from the reference program's by a relative error of at most 0.003.
Values may be sent and summed in bfloat16 or wider, within the bound.
No kernel may reach another device: no remote copies, remote signals or barrier semaphores. Data moves between devices by JAX's collectives and lax.ppermute only.
A program may use at most 128 MiB of HBM per device.

```python
import math
import jax
import jax.numpy as jnp
from jax import lax

HD = 128
KV_HEADS = 8
HEADS = 96
PREV = 3
GROUP = 12
TOK_DEV = 256
SPAN = 128
BLOCKS = 16
TOKENS = 4096


def draw_keys(key, part):
    shape_keys = (TOKENS, KV_HEADS * HD)
    base = jnp.clip(jax.random.normal(jax.random.fold_in(key, 11), shape_keys, jnp.float32), -4.0, 4.0)
    return base.astype(jnp.bfloat16)


def draw_queries(key, part):
    shape_queries = (TOKENS, HEADS * HD)
    base = jnp.clip(3.0 * jax.random.normal(jax.random.fold_in(key, 21), shape_queries, jnp.float32), -12.0, 12.0)
    return base.astype(jnp.bfloat16)


def shard_levels(stream_key, dims, cuts, smallest, top_value):
    factor_of = 1.0
    for position, shards_of in cuts:
        draws = jax.random.uniform(jax.random.fold_in(jax.random.fold_in(stream_key, 6), position), (shards_of,), jnp.float32, smallest / len(cuts), top_value / len(cuts))
        factor_of = factor_of * jnp.repeat(jnp.exp(draws), dims[position] // shards_of).reshape((-1,) + (1,) * (len(dims) - 1 - position))
    return factor_of


def centred(stream_key, dims, scale, limit, cuts=(), held_as=jnp.bfloat16):
    level = shard_levels(stream_key, dims, cuts, -0.22, 0.18) if cuts else 1.0
    values = jax.random.normal(stream_key, dims, jnp.float32) * scale * level
    return jnp.minimum(jnp.maximum(values, -limit), limit).astype(held_as)


def setup_inputs(seed: int = 0) -> dict:
    key_of = jax.random.split(jax.random.key(seed), 5)
    queries = draw_queries(jax.random.fold_in(key_of[4], 71), 0)
    keys = draw_keys(jax.random.fold_in(key_of[4], 71), 0)
    values = centred(key_of[2], (TOKENS, KV_HEADS * HD), 1.0, 6.0, ((0, 32),))
    block_order = jax.random.permutation(key_of[3], BLOCKS).astype(jnp.int32)
    return {"queries": queries, "keys": keys, "values": values, "block_order": block_order}


MASKED_SCORE = -1e+30

def token_positions(block_order):
    row_ids = jnp.arange(TOKENS, dtype=jnp.int32)
    owner_block = row_ids // TOK_DEV
    within = row_ids % TOK_DEV
    leading = block_order[owner_block].astype(jnp.int32)
    early_pos = leading * SPAN + within
    late_pos = (2 * BLOCKS - 1 - leading) * SPAN + within - SPAN
    return jnp.where(within < SPAN, early_pos, late_pos).astype(jnp.int32)

def reference(queries, keys, values, block_order):
    token_pos = token_positions(block_order)
    key_blocks = keys.astype(jnp.float32).reshape(BLOCKS, TOK_DEV, KV_HEADS, HD)
    value_blocks = values.astype(jnp.float32).reshape(BLOCKS, TOK_DEV, KV_HEADS, HD)
    pos_blocks = token_pos.reshape(BLOCKS, TOK_DEV)
    query_rows = math.gcd(TOK_DEV, 64)
    grouped = queries.reshape(BLOCKS, TOK_DEV // query_rows, query_rows, KV_HEADS, GROUP, HD)
    query_pos = token_pos.reshape(BLOCKS, TOK_DEV // query_rows, query_rows)
    score_scale = 1.0 / math.sqrt(HD)

    def per_block(inputs_block):
        block_id, query_set, pos_set = inputs_block
        window = (block_id - jnp.arange(PREV + 1, dtype=jnp.int32)) % BLOCKS
        window_keys = key_blocks[window].reshape((PREV + 1) * TOK_DEV, KV_HEADS, HD)
        window_values = value_blocks[window].reshape((PREV + 1) * TOK_DEV, KV_HEADS, HD)
        window_pos = pos_blocks[window].reshape((PREV + 1) * TOK_DEV)

        def attend(inputs_pair):
            query_block, query_here = inputs_pair
            scores = jnp.einsum('tkgd,skd->tkgs', query_block.astype(jnp.float32), window_keys) * score_scale
            visible = window_pos[None, None, None, :] <= query_here[:, None, None, None]
            row_max = lax.optimization_barrier(jnp.max(jnp.where(visible, scores, MASKED_SCORE), axis=-1, keepdims=True))
            exp_scores = jnp.where(visible, jnp.exp(scores - row_max), 0.0)
            denominator = lax.optimization_barrier(jnp.sum(exp_scores, axis=-1))
            rounded = lax.optimization_barrier(exp_scores.astype(jnp.bfloat16))
            weights = rounded.astype(jnp.float32)
            numerator = jnp.einsum('tkgs,skd->tkgd', weights, window_values)
            result = numerator / denominator[..., None]
            return result.astype(jnp.bfloat16).reshape(query_rows, HEADS * HD)
        return lax.map(attend, (query_set, pos_set))
    block_ids = jnp.arange(BLOCKS, dtype=jnp.int32)
    attended = lax.map(per_block, (block_ids, grouped, query_pos))
    return attended.reshape(TOKENS, HEADS * HD)
```

```python
import functools
import math

import jax
import jax.numpy as jnp
from jax import lax
from jax.experimental import pallas as pl
from jax.experimental.pallas import tpu as pltpu
from jax.sharding import PartitionSpec as P

HD = 128
PREV = 3


MASKED_SCORE = -1e30


def passed_along(value, axis, steps):
    count = lax.axis_size(axis)
    pairs = [(source, (source + steps) % count) for source in range(count)]
    return lax.ppermute(value, axis, pairs)


def block_positions(block_order, block_index, first_row, count, span_rows):
    block_total = block_order.shape[0]
    leading = jnp.sum(
        jnp.where(jnp.arange(block_total, dtype=jnp.int32) == block_index, block_order, 0)
    )
    row_ids = first_row + jnp.arange(count, dtype=jnp.int32)
    return jnp.where(
        row_ids < span_rows,
        leading * span_rows + row_ids,
        (2 * block_total - 1 - leading) * span_rows + row_ids - span_rows,
    )


def update(carried, queries_h, query_pos, key_part, value_part, key_pos):
    piece_rows = key_part.shape[0]
    block_rows = math.gcd(piece_rows, 256)
    block_count = piece_rows // block_rows
    score_scale = 1.0 / math.sqrt(queries_h.shape[-1])
    key_blocks = key_part.reshape(block_count, block_rows, key_part.shape[1], key_part.shape[2])
    value_blocks = value_part.reshape(
        block_count, block_rows, value_part.shape[1], value_part.shape[2]
    )
    pos_blocks = key_pos.reshape(block_count, block_rows)

    def advance(running, blocks_in):
        running_max, running_sum, numerator = running
        key_block, value_block, pos_block = blocks_in
        scores = (
            jnp.einsum("tkgd,skd->tkgs", queries_h, key_block, preferred_element_type=jnp.float32)
            * score_scale
        )
        visible = pos_block[None, None, None, :] <= query_pos[:, None, None, None]
        block_max = jnp.max(jnp.where(visible, scores, MASKED_SCORE), axis=-1)
        new_max = jnp.maximum(running_max, block_max)
        exp_scores = jnp.where(visible, jnp.exp(scores - new_max[..., None]), 0.0)
        rescale = jnp.exp(running_max - new_max)
        running_sum = running_sum * rescale + jnp.sum(exp_scores, axis=-1)
        weights = exp_scores.astype(jnp.bfloat16)
        numerator = numerator * rescale[..., None] + jnp.einsum(
            "tkgs,skd->tkgd", weights, value_block, preferred_element_type=jnp.float32
        )
        return ((new_max, running_sum, numerator), None)

    final_state, _ = lax.scan(advance, carried, (key_blocks, value_blocks, pos_blocks))
    return final_state


def general_device(queries, keys, values, block_order):
    block_total = block_order.shape[0]
    ctx_index = lax.axis_index("ctx")
    local_k, local_v = (
        lax.all_gather(keys, "tp", axis=0, tiled=True),
        lax.all_gather(values, "tp", axis=0, tiled=True),
    )
    first_row = lax.axis_index("tp") * queries.shape[0]
    token_rows = queries.shape[0]
    block_rows = local_k.shape[0]
    span_rows = block_rows // 2
    kv_local = local_k.shape[1] // HD
    group_size = queries.shape[1] // (HD * kv_local)
    queries_h = queries.reshape(token_rows, kv_local, group_size, HD)
    query_pos = block_positions(block_order, ctx_index, first_row, token_rows, span_rows)
    own_pair = jnp.stack(
        [local_k.reshape(block_rows, kv_local, HD), local_v.reshape(block_rows, kv_local, HD)]
    )
    state = (
        jnp.full((token_rows, kv_local, group_size), MASKED_SCORE, jnp.float32),
        jnp.zeros((token_rows, kv_local, group_size), jnp.float32),
        jnp.zeros((token_rows, kv_local, group_size, HD), jnp.float32),
    )
    own_pos = block_positions(block_order, ctx_index, 0, block_rows, span_rows)
    state = update(state, queries_h, query_pos, own_pair[0], own_pair[1], own_pos)
    moving = own_pair
    for step in range(1, PREV + 1):
        moving = passed_along(moving, "ctx", 1)
        source = (ctx_index - step) % block_total
        source_pos = block_positions(block_order, source, 0, block_rows, span_rows)
        state = update(state, queries_h, query_pos, moving[0], moving[1], source_pos)
    running_max, running_sum, numerator = state
    attended = (numerator / running_sum[..., None]).astype(jnp.bfloat16)
    attended = attended.reshape(token_rows, kv_local * group_size * HD)
    return attended


ROW_BLOCK = 4


def scored(left, right):
    return lax.dot_general(
        left, right, (((1,), (1,)), ((), ())), preferred_element_type=jnp.float32
    )


def weighed(left, right):
    return lax.dot_general(
        left, right, (((1,), (0,)), ((), ())), preferred_element_type=jnp.float32
    )


def attention_kernel(bias_ref, queries_ref, *refs, tiles, group, own, first, last):
    pairs, refs = refs[:tiles], refs[tiles:]
    if not first:
        (sum_in, stat_in), refs = refs[:2], refs[2:]
    rows = queries_ref.shape[0]
    scale = math.log2(math.e) / math.sqrt(HD)
    key_rows = jnp.concatenate([pair[:rows] for pair in pairs], axis=0)
    value_cols = jnp.concatenate([pair[rows:].T for pair in pairs], axis=1)
    value_cols = jnp.concatenate(
        [value_cols, jnp.ones((16, value_cols.shape[1]), jnp.bfloat16)], axis=0
    )
    if own:
        key_ids = lax.broadcasted_iota(jnp.int32, (rows, rows), 0)
        row_ids = lax.broadcasted_iota(jnp.int32, (rows, rows), 1)
        causal = jnp.where(key_ids <= row_ids, 0.0, MASKED_SCORE).astype(jnp.float32)
        causal = jnp.concatenate([causal] * ROW_BLOCK, axis=1)

    def span(head):
        return slice(head * rows, (head + ROW_BLOCK) * rows)

    def scores(head):
        block = jnp.concatenate(
            [queries_ref[:, (head + i) * HD : (head + i + 1) * HD] for i in range(ROW_BLOCK)], axis=0
        )
        product = scored(key_rows, block)
        parts = [
            product[t * rows : (t + 1) * rows] + (causal if own and t == 0 else bias_ref[t])
            for t in range(tiles)
        ]
        top = parts[0]
        for part in parts[1:]:
            top = jnp.maximum(top, part)
        top = jnp.max(top, axis=0, keepdims=True)
        if not first:
            top = jnp.maximum(top, stat_in[0:1, span(head)])
        return parts, top

    def finish(head, parts, top):
        weights = jnp.concatenate(
            [jnp.exp2((part - top) * scale).astype(jnp.bfloat16) for part in parts], axis=0
        )
        product = weighed(value_cols, weights)
        total, numerator = product[HD : HD + 1], product[:HD]
        if not first:
            rescale = jnp.exp2((stat_in[0:1, span(head)] - top) * scale)
            total = total + stat_in[1:2, span(head)] * rescale
            numerator = numerator + sum_in[:, span(head)] * rescale
        if last:
            (out_ref,) = refs
            result = (numerator / total).T.astype(jnp.bfloat16)
            for i in range(ROW_BLOCK):
                out_ref[:, (head + i) * HD : (head + i + 1) * HD] = result[i * rows : (i + 1) * rows]
        else:
            sum_out, stat_out = refs
            sum_out[:, span(head)] = numerator
            stat_out[0:1, span(head)] = top
            stat_out[1:2, span(head)] = total

    heads = list(range(0, group, ROW_BLOCK))
    ahead = scores(heads[0])
    for index, head in enumerate(heads):
        now = ahead
        if index + 1 < len(heads):
            ahead = scores(heads[index + 1])
        finish(head, *now)


def attend(bias, queries, pairs, state, own, last):
    rows, width = queries.shape
    kv_local = pairs[0].shape[1] // HD
    group = width // (HD * kv_local)
    tiles = len(pairs)
    queries_spec = pl.BlockSpec((rows, group * HD), lambda h, b: (0, h))
    pair_spec = pl.BlockSpec((2 * rows, HD), lambda h, b: (0, h))
    sum_spec = pl.BlockSpec((HD, group * rows), lambda h, b: (0, h))
    stat_spec = pl.BlockSpec((8, group * rows), lambda h, b: (0, h))
    in_specs = [queries_spec] + [pair_spec] * tiles
    if state is not None:
        in_specs += [sum_spec, stat_spec]
    if last:
        out_specs = queries_spec
        out_shape = jax.ShapeDtypeStruct(queries.shape, jnp.bfloat16)
    else:
        out_specs = (sum_spec, stat_spec)
        out_shape = tuple(
            jax.ShapeDtypeStruct((depth, kv_local * group * rows), jnp.float32) for depth in (HD, 8)
        )
    score_count = kv_local * group * rows * rows * tiles
    return pl.pallas_call(
        functools.partial(
            attention_kernel,
            tiles=tiles, group=group, own=own, first=state is None, last=last,
        ),
        grid_spec=pltpu.PrefetchScalarGridSpec(
            num_scalar_prefetch=1, grid=(kv_local,), in_specs=in_specs, out_specs=out_specs
        ),
        out_shape=out_shape,
        cost_estimate=pl.CostEstimate(
            flops=4 * score_count * HD,
            bytes_accessed=4 * rows * width * 2,
            transcendentals=score_count,
        ),
    )(bias, queries, *pairs, *(state or ()))


def span_device(queries, keys, values, block_order):
    block_total = block_order.shape[0]
    ctx_index = lax.axis_index("ctx")
    tp_index = lax.axis_index("tp")

    def moved(value, target):
        pairs = []
        for block in range(block_total):
            for half in range(2):
                to_block, to_half = target(block, half)
                pairs.append((block * 2 + half, (to_block % block_total) * 2 + to_half))
        return lax.ppermute(value, ("ctx", "tp"), pairs)

    def across(block, half):
        return block, 1 - half

    def two_on(block, half):
        return block + 2, half

    def to_next_pair(block, half):
        return block + (3 if block % 2 else 1), half

    def swapped(block, half):
        return block ^ 1, half

    own = jnp.concatenate([keys, values], axis=0)
    other_0 = moved(own, across)
    same_2 = moved(own, two_on)
    same_a = moved(own, to_next_pair)
    other_2 = moved(same_2, across)
    same_b = moved(same_2, swapped)
    other_a = moved(other_0, to_next_pair)
    other_b = moved(other_2, swapped)

    even = ctx_index % 2 == 0
    step_a = jnp.where(even, 3, 1)
    step_b = jnp.where(even, 1, 3)

    def position(step, half):
        leading = block_order[(ctx_index - step) % block_total]
        return jnp.where(half == 0, leading, 2 * block_total - 1 - leading)

    query_span = position(0, tp_index)
    tiles = [
        (0, 0), (0, 1), (2, 0), (step_a, 0),
        (step_b, 0), (step_a, 1), (2, 1), (step_b, 1),
    ]
    spans = jnp.stack(
        [position(step, tp_index if flip == 0 else 1 - tp_index) for step, flip in tiles]
    )
    bias = jnp.where(spans < query_span, 0.0, MASKED_SCORE).astype(jnp.float32)
    state = attend(bias[:4], queries, [own, other_0, same_2, same_a], None, True, False)
    return attend(bias[4:], queries, [same_b, other_a, other_2, other_b], state, False, True)


def solution(mesh):
    block_total, halves = mesh.shape["ctx"], mesh.shape["tp"]

    def per_device(queries, keys, values, block_order):
        rows = queries.shape[0]
        group = queries.shape[1] // keys.shape[1]
        fits = halves == 2 and block_total % 2 == 0 and block_total > PREV and rows == HD
        if fits and group % ROW_BLOCK == 0 and block_order.shape[0] == block_total:
            return span_device(queries, keys, values, block_order)
        return general_device(queries, keys, values, block_order)

    return jax.shard_map(
        per_device,
        mesh=mesh,
        in_specs=(P(("ctx", "tp"), None), P(("ctx", "tp"), None), P(("ctx", "tp"), None), P()),
        out_specs=P(("ctx", "tp"), None),
        check_vma=False,
    )
```

```python
import functools
import math

import jax
import jax.numpy as jnp
from jax import lax
from jax.experimental import pallas as pl
from jax.experimental.pallas import tpu as pltpu
from jax.sharding import PartitionSpec as P


HD = 128
PREV = 3


MASKED_SCORE = -1e30


def passed_along(value, axis, steps):
    count = lax.axis_size(axis)
    pairs = [(source, (source + steps) % count) for source in range(count)]
    return lax.ppermute(value, axis, pairs)


def block_positions(block_order, block_index, first_row, count, span_rows):
    block_total = block_order.shape[0]
    leading = jnp.sum(
        jnp.where(jnp.arange(block_total, dtype=jnp.int32) == block_index, block_order, 0)
    )
    row_ids = first_row + jnp.arange(count, dtype=jnp.int32)
    return jnp.where(
        row_ids < span_rows,
        leading * span_rows + row_ids,
        (2 * block_total - 1 - leading) * span_rows + row_ids - span_rows,
    )


def update(carried, queries_h, query_pos, key_part, value_part, key_pos):
    piece_rows = key_part.shape[0]
    block_rows = math.gcd(piece_rows, 256)
    block_count = piece_rows // block_rows
    score_scale = 1.0 / math.sqrt(queries_h.shape[-1])
    key_blocks = key_part.reshape(block_count, block_rows, key_part.shape[1], key_part.shape[2])
    value_blocks = value_part.reshape(
        block_count, block_rows, value_part.shape[1], value_part.shape[2]
    )
    pos_blocks = key_pos.reshape(block_count, block_rows)

    def advance(running, blocks_in):
        running_max, running_sum, numerator = running
        key_block, value_block, pos_block = blocks_in
        scores = (
            jnp.einsum("tkgd,skd->tkgs", queries_h, key_block, preferred_element_type=jnp.float32)
            * score_scale
        )
        visible = pos_block[None, None, None, :] <= query_pos[:, None, None, None]
        block_max = jnp.max(jnp.where(visible, scores, MASKED_SCORE), axis=-1)
        new_max = jnp.maximum(running_max, block_max)
        exp_scores = jnp.where(visible, jnp.exp(scores - new_max[..., None]), 0.0)
        rescale = jnp.exp(running_max - new_max)
        running_sum = running_sum * rescale + jnp.sum(exp_scores, axis=-1)
        weights = exp_scores.astype(jnp.bfloat16)
        numerator = numerator * rescale[..., None] + jnp.einsum(
            "tkgs,skd->tkgd", weights, value_block, preferred_element_type=jnp.float32
        )
        return ((new_max, running_sum, numerator), None)

    final_state, _ = lax.scan(advance, carried, (key_blocks, value_blocks, pos_blocks))
    return final_state


def general_device(queries, keys, values, block_order):
    block_total = block_order.shape[0]
    ctx_index = lax.axis_index("ctx")
    local_k, local_v = (
        lax.all_gather(keys, "tp", axis=0, tiled=True),
        lax.all_gather(values, "tp", axis=0, tiled=True),
    )
    first_row = lax.axis_index("tp") * queries.shape[0]
    token_rows = queries.shape[0]
    block_rows = local_k.shape[0]
    span_rows = block_rows // 2
    kv_local = local_k.shape[1] // HD
    group_size = queries.shape[1] // (HD * kv_local)
    queries_h = queries.reshape(token_rows, kv_local, group_size, HD)
    query_pos = block_positions(block_order, ctx_index, first_row, token_rows, span_rows)
    own_pair = jnp.stack(
        [local_k.reshape(block_rows, kv_local, HD), local_v.reshape(block_rows, kv_local, HD)]
    )
    state = (
        jnp.full((token_rows, kv_local, group_size), MASKED_SCORE, jnp.float32),
        jnp.zeros((token_rows, kv_local, group_size), jnp.float32),
        jnp.zeros((token_rows, kv_local, group_size, HD), jnp.float32),
    )
    own_pos = block_positions(block_order, ctx_index, 0, block_rows, span_rows)
    state = update(state, queries_h, query_pos, own_pair[0], own_pair[1], own_pos)
    moving = own_pair
    for step in range(1, PREV + 1):
        moving = passed_along(moving, "ctx", 1)
        source = (ctx_index - step) % block_total
        source_pos = block_positions(block_order, source, 0, block_rows, span_rows)
        state = update(state, queries_h, query_pos, moving[0], moving[1], source_pos)
    _, running_sum, numerator = state
    attended = (numerator / running_sum[..., None]).astype(jnp.bfloat16)
    attended = attended.reshape(token_rows, kv_local * group_size * HD)
    return attended


ROW_BLOCK = 6
PARTS = 2
VMEM_LIMIT = 32 * 2**20


def scored(left, right):
    return lax.dot_general(
        left, right, (((1,), (1,)), ((), ())), preferred_element_type=jnp.float32
    )


def weighed(left, right):
    return lax.dot_general(
        left, right, (((1,), (0,)), ((), ())), preferred_element_type=jnp.float32
    )


def attention_kernel(order_ref, queries_ref, *refs, tiles, counts, parts, kv_total, own, first, last):
    refs = list(refs)
    spans = [[refs.pop(0) for _ in range(count)] for count in counts]
    state_in = {} if first else {part: (refs.pop(0), refs.pop(0)) for part in parts}
    rows = queries_ref.shape[0]
    group = queries_ref.shape[1] // (HD * kv_total)
    kv_part = kv_total // PARTS
    scale = math.log2(math.e) / math.sqrt(HD)
    ctx_index, tp_index = lax.axis_index("ctx"), lax.axis_index("tp")
    block_total = order_ref.shape[0]

    def position(back, half):
        leading = order_ref[lax.rem(ctx_index + block_total - back, block_total)]
        return jnp.where(half == 0, leading, 2 * block_total - 1 - leading)

    def bias(tile):
        even_back, odd_back, flip = tile
        back = jnp.where(lax.rem(ctx_index, 2) == 0, even_back, odd_back)
        half = 1 - tp_index if flip else tp_index
        return jnp.where(position(back, half) < position(0, tp_index), 0.0, MASKED_SCORE)

    biases = [0.0 if own and t == 0 else bias(tile) for t, tile in enumerate(tiles)]

    def pairs_of(head):
        kv_head = head // group
        found = []
        for arrays in spans:
            whole = arrays[0].shape[1] == kv_total * HD
            ref = arrays[0] if whole else arrays[parts.index(kv_head // kv_part)]
            at = (kv_head if whole else kv_head % kv_part) * HD
            found.append((ref, slice(at, at + HD)))
        return found

    def key_rows(head):
        return jnp.concatenate([ref[:rows, at] for ref, at in pairs_of(head)], axis=0)

    def value_cols(head):
        cols = jnp.concatenate([ref[rows:, at].T for ref, at in pairs_of(head)], axis=1)
        return jnp.concatenate([cols, jnp.ones((16, cols.shape[1]), jnp.bfloat16)], axis=0)

    if own:
        key_ids = lax.broadcasted_iota(jnp.int32, (rows, rows), 0)
        row_ids = lax.broadcasted_iota(jnp.int32, (rows, rows), 1)
        causal = jnp.where(key_ids <= row_ids, 0.0, MASKED_SCORE).astype(jnp.float32)
        causal = jnp.concatenate([causal] * ROW_BLOCK, axis=1)

    def held(state, head):
        part, inside = divmod(head, kv_part * group)
        return *state[part], slice(inside * rows, (inside + ROW_BLOCK) * rows)

    def scores(head):
        block = jnp.concatenate(
            [queries_ref[:, (head + i) * HD : (head + i + 1) * HD] for i in range(ROW_BLOCK)], axis=0
        )
        product = scored(key_rows(head), block)
        pieces = [product[t * rows : (t + 1) * rows] for t in range(len(tiles))]
        if own:
            pieces[0] = pieces[0] + causal
        tops = [jnp.max(piece, axis=0, keepdims=True) + b for piece, b in zip(pieces, biases)]
        if not first:
            _, stat, at = held(state_in, head)
            tops.append(stat[0:1, at])
        return pieces, functools.reduce(jnp.maximum, tops)

    def finish(head, pieces, top):
        weights = jnp.concatenate(
            [
                jnp.exp2((piece - (top - b)) * scale).astype(jnp.bfloat16)
                for piece, b in zip(pieces, biases)
            ],
            axis=0,
        )
        product = weighed(value_cols(head), weights)
        total, numerator = product[HD : HD + 1], product[:HD]
        if not first:
            sums, stat, at = held(state_in, head)
            rescale = jnp.exp2((stat[0:1, at] - top) * scale)
            total = total + stat[1:2, at] * rescale
            numerator = numerator + sums[:, at] * rescale
        if last:
            out_ref, rounded, sems = refs
            result = (numerator / total).T.astype(jnp.bfloat16)
            for i in range(ROW_BLOCK):
                rounded[:, (head + i) * HD : (head + i + 1) * HD] = result[i * rows : (i + 1) * rows]
            columns = slice(head * HD, (head + ROW_BLOCK) * HD)
            copies.append(
                pltpu.make_async_copy(
                    rounded.at[:, columns], out_ref.at[:, columns], sems.at[len(copies)]
                )
            )
            copies[-1].start()
        else:
            state_out = {part: refs[2 * i : 2 * i + 2] for i, part in enumerate(parts)}
            sums, stat, at = held(state_out, head)
            sums[:, at] = numerator
            stat[0:1, at] = top
            stat[1:2, at] = total

    copies = []
    part_heads = kv_part * group
    heads = [
        part * part_heads + inside for part in parts for inside in range(0, part_heads, ROW_BLOCK)
    ]
    ahead = scores(heads[0])
    for index, head in enumerate(heads):
        now = ahead
        if index + 1 < len(heads):
            ahead = scores(heads[index + 1])
        finish(head, *now)
    for copy in copies:
        copy.wait()


def attend(block_order, queries, kv_total, spans, state, parts, own=False, last=False):
    rows, width = queries.shape
    arrays = [list(held) if len(held) == 1 else [held[part] for part in parts] for held, _ in spans]
    operands = [array for held in arrays for array in held]
    operands += [] if state is None else [array for held in state for array in held]
    here = pl.BlockSpec(memory_space=pltpu.VMEM)
    if last:
        out_specs = pl.BlockSpec(memory_space=pl.ANY)
        out_shape = jax.ShapeDtypeStruct(queries.shape, jnp.bfloat16)
        scratch_shapes = [
            pltpu.VMEM(queries.shape, jnp.bfloat16),
            pltpu.SemaphoreType.DMA((width // (ROW_BLOCK * HD),)),
        ]
    else:
        out_specs = (here,) * (2 * len(parts))
        out_shape = tuple(
            jax.ShapeDtypeStruct((depth, width // HD * rows // PARTS), jnp.float32)
            for _ in parts
            for depth in (HD, 8)
        )
        scratch_shapes = []
    score_count = width // HD * rows * rows * len(spans) * len(parts) // PARTS
    result = pl.pallas_call(
        functools.partial(
            attention_kernel,
            tiles=[place for _, place in spans], counts=[len(held) for held in arrays],
            parts=parts, kv_total=kv_total, own=own, first=state is None, last=last,
        ),
        in_specs=[pl.BlockSpec(memory_space=pltpu.SMEM)] + [here] * (1 + len(operands)),
        out_specs=out_specs,
        scratch_shapes=scratch_shapes,
        out_shape=out_shape,
        compiler_params=pltpu.CompilerParams(vmem_limit_bytes=VMEM_LIMIT),
        cost_estimate=pl.CostEstimate(
            flops=4 * score_count * HD,
            bytes_accessed=4 * rows * width * 2,
            transcendentals=score_count,
        ),
    )(block_order, queries, *operands)
    return result if last else [result[2 * i : 2 * i + 2] for i in range(len(parts))]


def span_device(queries, keys, values, block_order):
    block_total = block_order.shape[0]
    rows, kv_width = keys.shape
    kv_total = kv_width // HD

    def moved(value, target):
        pairs = []
        for block in range(block_total):
            for half in range(2):
                to_block, to_half = target(block, half)
                pairs.append((block * 2 + half, (to_block % block_total) * 2 + to_half))
        return lax.ppermute(value, ("ctx", "tp"), pairs)

    def moved_parts(values_of, target):
        return [moved(value, target) for value in values_of]

    def across(block, half):
        return block, 1 - half

    def two_on(block, half):
        return block + 2, half

    def to_next_pair(block, half):
        return block + (3 if block % 2 else 1), half

    def swapped(block, half):
        return block ^ 1, half

    def packed(columns):
        return jnp.stack([keys[:, columns], values[:, columns]]).reshape(2 * rows, -1)

    width = kv_width // PARTS
    own = [packed(slice(part * width, (part + 1) * width)) for part in range(PARTS)]
    same_2 = moved_parts(own, two_on)
    other_0 = moved_parts(own, across)
    same_a = moved_parts(own, to_next_pair)
    other_2 = moved_parts(same_2, across)
    same_b = moved_parts(same_2, swapped)
    other_a = moved_parts(other_0, to_next_pair)
    other_b = moved_parts(other_2, swapped)
    everything = tuple(range(PARTS))
    spans = [(own, (0, 0, False))]
    state = attend(block_order, queries, kv_total, spans, None, everything, own=True)
    spans = [(other_0, (0, 0, True)), (same_2, (2, 2, False)), (same_b, (1, 3, False))]
    for part in everything:
        (state[part],) = attend(
            block_order, queries, kv_total, spans, [state[part]], (part,)
        )
    spans = [
        (same_a, (3, 1, False)),
        (other_a, (3, 1, True)),
        (other_2, (2, 2, True)),
        (other_b, (1, 3, True)),
    ]
    return attend(block_order, queries, kv_total, spans, state, everything, last=True)


def solution(mesh):
    block_total, halves = mesh.shape["ctx"], mesh.shape["tp"]
    in_pairs = halves == 2 and block_total % 2 == 0 and block_total > PREV

    def per_device(queries, keys, values, block_order):
        if in_pairs:
            return span_device(queries, keys, values, block_order)
        return general_device(queries, keys, values, block_order)

    return jax.shard_map(
        per_device,
        mesh=mesh,
        in_specs=(P(("ctx", "tp"), None), P(("ctx", "tp"), None), P(("ctx", "tp"), None), P()),
        out_specs=P(("ctx", "tp"), None),
        check_vma=False,
    )
```

```python
import functools
import math

import jax
import jax.numpy as jnp
from jax import lax
from jax.experimental import pallas as pl
from jax.experimental.pallas import tpu as pltpu
from jax.sharding import PartitionSpec as P


HD = 128
PREV = 3


MASKED_SCORE = -1e30


def passed_along(value, axis, steps):
    count = lax.axis_size(axis)
    pairs = [(source, (source + steps) % count) for source in range(count)]
    return lax.ppermute(value, axis, pairs)


def block_positions(block_order, block_index, first_row, count, span_rows):
    block_total = block_order.shape[0]
    leading = jnp.sum(
        jnp.where(jnp.arange(block_total, dtype=jnp.int32) == block_index, block_order, 0)
    )
    row_ids = first_row + jnp.arange(count, dtype=jnp.int32)
    return jnp.where(
        row_ids < span_rows,
        leading * span_rows + row_ids,
        (2 * block_total - 1 - leading) * span_rows + row_ids - span_rows,
    )


def update(carried, queries_h, query_pos, key_part, value_part, key_pos):
    piece_rows = key_part.shape[0]
    block_rows = math.gcd(piece_rows, 256)
    block_count = piece_rows // block_rows
    score_scale = 1.0 / math.sqrt(queries_h.shape[-1])
    key_blocks = key_part.reshape(block_count, block_rows, key_part.shape[1], key_part.shape[2])
    value_blocks = value_part.reshape(
        block_count, block_rows, value_part.shape[1], value_part.shape[2]
    )
    pos_blocks = key_pos.reshape(block_count, block_rows)

    def advance(running, blocks_in):
        running_max, running_sum, numerator = running
        key_block, value_block, pos_block = blocks_in
        scores = (
            jnp.einsum("tkgd,skd->tkgs", queries_h, key_block, preferred_element_type=jnp.float32)
            * score_scale
        )
        visible = pos_block[None, None, None, :] <= query_pos[:, None, None, None]
        block_max = jnp.max(jnp.where(visible, scores, MASKED_SCORE), axis=-1)
        new_max = jnp.maximum(running_max, block_max)
        exp_scores = jnp.where(visible, jnp.exp(scores - new_max[..., None]), 0.0)
        rescale = jnp.exp(running_max - new_max)
        running_sum = running_sum * rescale + jnp.sum(exp_scores, axis=-1)
        weights = exp_scores.astype(jnp.bfloat16)
        numerator = numerator * rescale[..., None] + jnp.einsum(
            "tkgs,skd->tkgd", weights, value_block, preferred_element_type=jnp.float32
        )
        return ((new_max, running_sum, numerator), None)

    final_state, _ = lax.scan(advance, carried, (key_blocks, value_blocks, pos_blocks))
    return final_state


def general_device(queries, keys, values, block_order):
    block_total = block_order.shape[0]
    ctx_index = lax.axis_index("ctx")
    local_k, local_v = (
        lax.all_gather(keys, "tp", axis=0, tiled=True),
        lax.all_gather(values, "tp", axis=0, tiled=True),
    )
    first_row = lax.axis_index("tp") * queries.shape[0]
    token_rows = queries.shape[0]
    block_rows = local_k.shape[0]
    span_rows = block_rows // 2
    kv_local = local_k.shape[1] // HD
    group_size = queries.shape[1] // (HD * kv_local)
    queries_h = queries.reshape(token_rows, kv_local, group_size, HD)
    query_pos = block_positions(block_order, ctx_index, first_row, token_rows, span_rows)
    own_pair = jnp.stack(
        [local_k.reshape(block_rows, kv_local, HD), local_v.reshape(block_rows, kv_local, HD)]
    )
    state = (
        jnp.full((token_rows, kv_local, group_size), MASKED_SCORE, jnp.float32),
        jnp.zeros((token_rows, kv_local, group_size), jnp.float32),
        jnp.zeros((token_rows, kv_local, group_size, HD), jnp.float32),
    )
    own_pos = block_positions(block_order, ctx_index, 0, block_rows, span_rows)
    state = update(state, queries_h, query_pos, own_pair[0], own_pair[1], own_pos)
    moving = own_pair
    for step in range(1, PREV + 1):
        moving = passed_along(moving, "ctx", 1)
        source = (ctx_index - step) % block_total
        source_pos = block_positions(block_order, source, 0, block_rows, span_rows)
        state = update(state, queries_h, query_pos, moving[0], moving[1], source_pos)
    _, running_sum, numerator = state
    attended = (numerator / running_sum[..., None]).astype(jnp.bfloat16)
    attended = attended.reshape(token_rows, kv_local * group_size * HD)
    return attended


ROW_BLOCK = 6
PARTS = 2
OWN_LIMIT = 44 * 2**20
VMEM_LIMIT = 32 * 2**20


def scored(left, right):
    return lax.dot_general(
        left, right, (((1,), (1,)), ((), ())), preferred_element_type=jnp.float32
    )


def weighed(left, right):
    return lax.dot_general(
        left, right, (((1,), (0,)), ((), ())), preferred_element_type=jnp.float32
    )


def attention_kernel(*refs, tiles, counts, parts, kv_total, own, first, last):
    refs = list(refs)
    order_ref = None if own else refs.pop(0)
    queries_ref = refs.pop(0)
    spans = [[refs.pop(0) for _ in range(count)] for count in counts]
    state_in = {} if first else {part: (refs.pop(0), refs.pop(0)) for part in parts}
    rows = queries_ref.shape[0]
    group = queries_ref.shape[1] // (HD * kv_total)
    kv_part = kv_total // PARTS
    scale = math.log2(math.e) / math.sqrt(HD)
    ctx_index, tp_index = lax.axis_index("ctx"), lax.axis_index("tp")

    def position(back, half):
        block_total = order_ref.shape[0]
        leading = order_ref[lax.rem(ctx_index + block_total - back, block_total)]
        return jnp.where(half == 0, leading, 2 * block_total - 1 - leading)

    def bias(tile):
        even_back, odd_back, flip = tile
        back = jnp.where(lax.rem(ctx_index, 2) == 0, even_back, odd_back)
        half = 1 - tp_index if flip else tp_index
        return jnp.where(position(back, half) < position(0, tp_index), 0.0, MASKED_SCORE)

    biases = [0.0 if own and t == 0 else bias(tile) for t, tile in enumerate(tiles)]

    def pairs_of(head):
        kv_head = head // group
        found = []
        for arrays in spans:
            whole = arrays[0].shape[1] == kv_total * HD
            ref = arrays[0] if whole else arrays[parts.index(kv_head // kv_part)]
            at = (kv_head if whole else kv_head % kv_part) * HD
            found.append((ref, slice(at, at + HD)))
        return found

    def key_rows(head):
        return jnp.concatenate([ref[:rows, at] for ref, at in pairs_of(head)], axis=0)

    def value_cols(head):
        cols = jnp.concatenate([ref[rows:, at].T for ref, at in pairs_of(head)], axis=1)
        return jnp.concatenate([cols, jnp.ones((16, cols.shape[1]), jnp.bfloat16)], axis=0)

    arrivals = {}
    if own:
        queries_far, (queries_ref, arrival_sems) = queries_ref, refs[-2:]
        for kv_head in range(kv_total):
            columns = slice(kv_head * group * HD, (kv_head + 1) * group * HD)
            arrivals[kv_head] = pltpu.make_async_copy(
                queries_far.at[:, columns], queries_ref.at[:, columns], arrival_sems.at[kv_head]
            )
            arrivals[kv_head].start()
        key_ids = lax.broadcasted_iota(jnp.int32, (rows, rows), 0)
        row_ids = lax.broadcasted_iota(jnp.int32, (rows, rows), 1)
        causal = jnp.where(key_ids <= row_ids, 0.0, MASKED_SCORE).astype(jnp.float32)
        causal = jnp.concatenate([causal] * ROW_BLOCK, axis=1)

    def held(state, head):
        part, inside = divmod(head, kv_part * group)
        return *state[part], slice(inside * rows, (inside + ROW_BLOCK) * rows)

    def scores(head):
        if head // group in arrivals:
            arrivals.pop(head // group).wait()
        block = jnp.concatenate(
            [queries_ref[:, (head + i) * HD : (head + i + 1) * HD] for i in range(ROW_BLOCK)], axis=0
        )
        product = scored(key_rows(head), block)
        pieces = [product[t * rows : (t + 1) * rows] for t in range(len(tiles))]
        if own:
            pieces[0] = pieces[0] + causal
        tops = [jnp.max(piece, axis=0, keepdims=True) + b for piece, b in zip(pieces, biases)]
        if not first:
            _, stat, at = held(state_in, head)
            tops.append(stat[0:1, at])
        return pieces, functools.reduce(jnp.maximum, tops)

    def finish(head, pieces, top):
        weights = jnp.concatenate(
            [
                jnp.exp2((piece - (top - b)) * scale).astype(jnp.bfloat16)
                for piece, b in zip(pieces, biases)
            ],
            axis=0,
        )
        product = weighed(value_cols(head), weights)
        total, numerator = product[HD : HD + 1], product[:HD]
        if not first:
            sums, stat, at = held(state_in, head)
            rescale = jnp.exp2((stat[0:1, at] - top) * scale)
            total = total + stat[1:2, at] * rescale
            numerator = numerator + sums[:, at] * rescale
        if last:
            out_ref, rounded, sems = refs
            result = (numerator / total).T.astype(jnp.bfloat16)
            for i in range(ROW_BLOCK):
                rounded[:, (head + i) * HD : (head + i + 1) * HD] = result[i * rows : (i + 1) * rows]
            columns = slice(head * HD, (head + ROW_BLOCK) * HD)
            copies.append(
                pltpu.make_async_copy(
                    rounded.at[:, columns], out_ref.at[:, columns], sems.at[len(copies)]
                )
            )
            copies[-1].start()
        else:
            state_out = {part: refs[2 * i : 2 * i + 2] for i, part in enumerate(parts)}
            sums, stat, at = held(state_out, head)
            sums[:, at] = numerator
            stat[0:1, at] = top
            stat[1:2, at] = total

    copies = []
    part_heads = kv_part * group
    heads = [
        part * part_heads + inside for part in parts for inside in range(0, part_heads, ROW_BLOCK)
    ]
    ahead = scores(heads[0])
    for index, head in enumerate(heads):
        now = ahead
        if index + 1 < len(heads):
            ahead = scores(heads[index + 1])
        finish(head, *now)
    for copy in copies:
        copy.wait()


def attend(block_order, queries, kv_total, spans, state, parts, own=False, last=False):
    rows, width = queries.shape
    arrays = [list(held) if len(held) == 1 else [held[part] for part in parts] for held, _ in spans]
    operands = [array for held in arrays for array in held]
    operands += [] if state is None else [array for held in state for array in held]
    here = pl.BlockSpec(memory_space=pltpu.VMEM)
    if last:
        out_specs = pl.BlockSpec(memory_space=pl.ANY)
        out_shape = jax.ShapeDtypeStruct(queries.shape, jnp.bfloat16)
        scratch_shapes = [
            pltpu.VMEM(queries.shape, jnp.bfloat16),
            pltpu.SemaphoreType.DMA((width // (ROW_BLOCK * HD),)),
        ]
    else:
        out_specs = (here,) * (2 * len(parts))
        out_shape = tuple(
            jax.ShapeDtypeStruct((depth, width // HD * rows // PARTS), jnp.float32)
            for _ in parts
            for depth in (HD, 8)
        )
        scratch_shapes = []
        if own:
            out_specs += (here,)
            out_shape += (jax.ShapeDtypeStruct(queries.shape, jnp.bfloat16),)
            scratch_shapes = [pltpu.SemaphoreType.DMA((kv_total,))]
    in_specs = [here] * (1 + len(operands))
    operands.insert(0, queries)
    if own:
        in_specs[0] = pl.BlockSpec(memory_space=pltpu.HBM)
    else:
        in_specs.insert(0, pl.BlockSpec(memory_space=pltpu.SMEM))
        operands.insert(0, block_order)
    score_count = width // HD * rows * rows * len(spans) * len(parts) // PARTS
    result = pl.pallas_call(
        functools.partial(
            attention_kernel,
            tiles=[place for _, place in spans], counts=[len(held) for held in arrays],
            parts=parts, kv_total=kv_total, own=own, first=state is None, last=last,
        ),
        in_specs=in_specs,
        out_specs=out_specs,
        scratch_shapes=scratch_shapes,
        out_shape=out_shape,
        compiler_params=pltpu.CompilerParams(vmem_limit_bytes=OWN_LIMIT if own else VMEM_LIMIT),
        cost_estimate=pl.CostEstimate(
            flops=4 * score_count * HD,
            bytes_accessed=4 * rows * width * 2,
            transcendentals=score_count,
        ),
    )(*operands)
    if last:
        return result
    states = [result[2 * i : 2 * i + 2] for i in range(len(parts))]
    return (states, result[-1]) if own else states


def span_device(queries, keys, values, block_order):
    block_total = block_order.shape[0]
    rows, kv_width = keys.shape
    kv_total = kv_width // HD

    def moved(value, target):
        pairs = []
        for block in range(block_total):
            for half in range(2):
                to_block, to_half = target(block, half)
                pairs.append((block * 2 + half, (to_block % block_total) * 2 + to_half))
        return lax.ppermute(value, ("ctx", "tp"), pairs)

    def moved_parts(values_of, target):
        return [moved(value, target) for value in values_of]

    def across(block, half):
        return block, 1 - half

    def two_on(block, half):
        return block + 2, half

    def to_next_pair(block, half):
        return block + (3 if block % 2 else 1), half

    def swapped(block, half):
        return block ^ 1, half

    def packed(columns):
        return jnp.stack([keys[:, columns], values[:, columns]]).reshape(2 * rows, -1)

    width = kv_width // PARTS
    own = [packed(slice(part * width, (part + 1) * width)) for part in range(PARTS)]
    same_2 = moved_parts(own, two_on)
    other_0 = moved_parts(own, across)
    same_a = moved_parts(own, to_next_pair)
    other_2 = moved_parts(same_2, across)
    same_b = moved_parts(same_2, swapped)
    other_a = moved_parts(other_0, to_next_pair)
    other_b = moved_parts(other_2, swapped)
    everything = tuple(range(PARTS))
    spans = [(own, (0, 0, False))]
    state, queries = attend(block_order, queries, kv_total, spans, None, everything, own=True)
    spans = [(other_0, (0, 0, True)), (same_2, (2, 2, False)), (same_b, (1, 3, False))]
    for part in everything:
        (state[part],) = attend(block_order, queries, kv_total, spans, [state[part]], (part,))
    spans = [
        (same_a, (3, 1, False)),
        (other_a, (3, 1, True)),
        (other_2, (2, 2, True)),
        (other_b, (1, 3, True)),
    ]
    return attend(block_order, queries, kv_total, spans, state, everything, last=True)


def solution(mesh):
    block_total, halves = mesh.shape["ctx"], mesh.shape["tp"]
    in_pairs = halves == 2 and block_total % 2 == 0 and block_total > PREV

    def per_device(queries, keys, values, block_order):
        if in_pairs:
            return span_device(queries, keys, values, block_order)
        return general_device(queries, keys, values, block_order)

    return jax.shard_map(
        per_device,
        mesh=mesh,
        in_specs=(P(("ctx", "tp"), None), P(("ctx", "tp"), None), P(("ctx", "tp"), None), P()),
        out_specs=P(("ctx", "tp"), None),
        check_vma=False,
    )
```
